8 devices in a mesh: data: 2 (over z, y), seq: 4 (over x, core).
Axes of the slice: x: 2, y: 2, z: 1, core: 2. Of those that a mesh axis runs over, the one named last changes fastest.
Arguments:
- x: bfloat16 [32768, 2048], P(('data', 'seq')), parts along dimension 0
- dout: bfloat16 [32768, 2048], P(('data', 'seq')), parts along dimension 0
- W_in: bfloat16 [2048, 8512], replicated
- conv_w: float32 [4, 4352], replicated
- conv_b: float32 [4352], replicated
- dt_bias: float32 [64], replicated
- A_log: float32 [64], replicated
- D_skip: float32 [64], replicated
- norm_w: float32 [4096], replicated
- W_out: bfloat16 [4096, 2048], replicated
Outputs:
- output 1: bfloat16 [32768, 2048], P(('data', 'seq')), parts along dimension 0
- output 2: bfloat16 [4096, 8512], P('data'), parts along dimension 0
- output 3: float32 [8, 4352], P('data'), parts along dimension 0
- output 4: float32 [8704], P('data'), parts along dimension 0
- output 5: float32 [128], P('data'), parts along dimension 0
- output 6: float32 [128], P('data'), parts along dimension 0
- output 7: float32 [128], P('data'), parts along dimension 0
- output 8: float32 [8192], P('data'), parts along dimension 0
- output 9: bfloat16 [8192, 2048], P('data'), parts along dimension 0
There are 2 independent parts. The reference program is written for one: setup_inputs(seed, part) draws one part's arguments, and reference() takes and returns one part's arrays. A program takes and returns all parts, laid end to end along the dimension named above; an argument that names none is the same for every part.
All inputs are finite; a program needn't handle non-finite values.
Results may differ from the reference program's by a relative error of at most 0.00793302.
Values are sent between devices in bfloat16 or wider.
A program may use at most 1 GiB of HBM per device.

```python
import jax
import jax.numpy as jnp
from jax import lax

SEQ = 4
TOKENS_DEV = 4096
D_MODEL = 2048
HEADS = 64
HEADDIM = 64
NGROUPS = 1
DSTATE = 128
CHUNK = 256
KCONV = 4
T = SEQ * TOKENS_DEV
D_INNER = HEADS * HEADDIM
GN = NGROUPS * DSTATE
CONV_DIM = D_INNER + 2 * GN
PROJ = 2 * D_INNER + 2 * GN + HEADS
HG = HEADS // NGROUPS
EPS = 1e-5


def setup_inputs(seed: int = 0, part: int = 0) -> dict:
    f32 = jnp.float32
    key = jax.random.key(seed)
    kx, kd = jax.random.split(jax.random.fold_in(key, part))
    k = jax.random.split(key, 8)
    x = jax.random.normal(kx, (T, D_MODEL), f32).astype(jnp.bfloat16)
    dout = jax.random.normal(kd, (T, D_MODEL), f32).astype(jnp.bfloat16)
    W_in = (jax.random.normal(k[0], (D_MODEL, PROJ), f32) * D_MODEL ** -0.5).astype(jnp.bfloat16)
    conv_w = jax.random.normal(k[1], (KCONV, CONV_DIM), f32) * 0.5
    conv_b = jax.random.normal(k[2], (CONV_DIM,), f32) * 0.2
    dt0 = jax.random.uniform(k[3], (HEADS,), f32, 0.02, 0.1)
    dt_bias = jnp.log(jnp.expm1(dt0))
    decay = jax.random.uniform(k[4], (HEADS,), f32, 0.2, 1.8)
    A_log = jnp.log(decay / (1.5 * dt0 * TOKENS_DEV))
    D_skip = jax.random.uniform(k[5], (HEADS,), f32, 0.5, 1.5)
    norm_w = 1.0 + 0.2 * jax.random.normal(k[6], (D_INNER,), f32)
    W_out = (jax.random.normal(k[7], (D_INNER, D_MODEL), f32) * D_INNER ** -0.5).astype(jnp.bfloat16)
    return {'x': x, 'dout': dout, 'W_in': W_in, 'conv_w': conv_w, 'conv_b': conv_b, 'dt_bias': dt_bias,
            'A_log': A_log, 'D_skip': D_skip, 'norm_w': norm_w, 'W_out': W_out}


def _ssd(X, Bm, Cm, dt, a):
    f32 = jnp.float32
    nc = T // CHUNK
    causal = jnp.tril(jnp.ones((CHUNK, CHUNK), bool))

    def step(h, inp):
        xq, bq, cq, dq, aq = inp
        acs = jnp.cumsum(aq, 0)
        ae = acs[-1]
        bh = jnp.repeat(bq.astype(f32), HG, axis=1)
        ch = jnp.repeat(cq.astype(f32), HG, axis=1)
        cb = jnp.repeat(jnp.einsum('qgn,sgn->gqs', cq.astype(f32), bq.astype(f32)), HG, axis=0)
        at = acs.T
        seg = jnp.where(causal, at[:, :, None] - at[:, None, :], 0.0)
        w = jnp.where(causal, jnp.exp(seg), 0.0) * dq.T[:, None, :]
        sc = (cb * w).astype(jnp.bfloat16)
        y = jnp.einsum('hqs,shp->qhp', sc.astype(f32), xq.astype(f32))
        hb = h.astype(jnp.bfloat16).astype(f32)
        y = y + jnp.exp(acs)[:, :, None] * jnp.einsum('qhn,hpn->qhp', ch, hb)
        xw = (xq.astype(f32) * (dq * jnp.exp(ae - acs))[:, :, None]).astype(jnp.bfloat16)
        st = jnp.einsum('qhn,qhp->hpn', bh, xw.astype(f32))
        return jnp.exp(ae)[:, None, None] * h + st, y

    xs = (X.reshape(nc, CHUNK, HEADS, HEADDIM), Bm.reshape(nc, CHUNK, NGROUPS, DSTATE),
          Cm.reshape(nc, CHUNK, NGROUPS, DSTATE), dt.reshape(nc, CHUNK, HEADS), a.reshape(nc, CHUNK, HEADS))
    _, y = lax.scan(jax.checkpoint(step), jnp.zeros((HEADS, HEADDIM, DSTATE), f32), xs)
    return y.reshape(T, HEADS, HEADDIM)


def _forward(x, W_in, conv_w, conv_b, dt_bias, A_log, D_skip, norm_w, W_out):
    f32 = jnp.float32
    zx = jnp.dot(x, W_in, preferred_element_type=f32).astype(jnp.bfloat16)
    z = zx[:, :D_INNER].astype(f32)
    xbc = zx[:, D_INNER:D_INNER + CONV_DIM].astype(f32)
    dtr = zx[:, D_INNER + CONV_DIM:].astype(f32)
    xp = jnp.concatenate([jnp.zeros((KCONV - 1, CONV_DIM), f32), xbc], 0)
    u = conv_b + sum(conv_w[j] * xp[KCONV - 1 - j:KCONV - 1 - j + T] for j in range(KCONV))
    xc = (u * jax.nn.sigmoid(u)).astype(jnp.bfloat16)
    X = xc[:, :D_INNER].reshape(T, HEADS, HEADDIM)
    Bm = xc[:, D_INNER:D_INNER + GN].reshape(T, NGROUPS, DSTATE)
    Cm = xc[:, D_INNER + GN:].reshape(T, NGROUPS, DSTATE)
    dt = jax.nn.softplus(dtr + dt_bias)
    a = -jnp.exp(A_log) * dt
    y = _ssd(X, Bm, Cm, dt, a) + D_skip[:, None] * X.astype(f32)
    y = y.reshape(T, D_INNER) * (z * jax.nn.sigmoid(z))
    yg = y.reshape(T, NGROUPS, D_INNER // NGROUPS)
    yg = yg * lax.rsqrt(jnp.mean(yg * yg, -1, keepdims=True) + EPS)
    yn = (yg.reshape(T, D_INNER) * norm_w).astype(jnp.bfloat16)
    return jnp.dot(yn, W_out, preferred_element_type=f32).astype(jnp.bfloat16)


def reference(x, dout, W_in, conv_w, conv_b, dt_bias, A_log, D_skip, norm_w, W_out):
    _, vjp = jax.vjp(_forward, x, W_in, conv_w, conv_b, dt_bias, A_log, D_skip, norm_w, W_out)
    dx, dW_in, dconv_w, dconv_b, ddt_bias, dA_log, dD_skip, dnorm_w, dW_out = vjp(dout)
    return (dx, dW_in, dconv_w, dconv_b, ddt_bias, dA_log, dD_skip, dnorm_w, dW_out)
```

```python
import jax
import jax.numpy as jnp
from jax import lax
from jax.experimental import pallas as pl
from jax.experimental.pallas import tpu as pltpu
from jax.sharding import PartitionSpec as P

Q = 256
N = 128
H = 64
E = 4096
CD = E + 2 * N
PX = CD + H
KCONV = 4
EPS = 1e-5
LOG2E = 1.4426950408889634
F32 = jnp.float32
BF16 = jnp.bfloat16
HI = lax.Precision.HIGHEST
HB = 128


def _dot(a, b):
    return lax.dot_general(a, b, (((1,), (0,)), ((), ())), preferred_element_type=F32)


def _tn(a, b):
    return lax.dot_general(a, b, (((0,), (0,)), ((), ())), preferred_element_type=F32)


def _nt(a, b):
    return lax.dot_general(a, b, (((1,), (1,)), ((), ())), preferred_element_type=F32)


def _lanes(j, w):
    return pl.ds(pl.multiple_of(j * w, w), w)


def _iota(shape, d):
    return lax.broadcasted_iota(jnp.int32, shape, d)


def _split3(v):
    hi = v.astype(BF16).astype(F32)
    mid = (v - hi).astype(BF16).astype(F32)
    lo = v - hi - mid
    return jnp.concatenate([hi, mid, lo, jnp.zeros_like(v)], 1).astype(BF16)


def _split2(v):
    hi = v.astype(BF16)
    return hi, (v - hi.astype(F32)).astype(BF16)


def _softplus(v):
    return jnp.maximum(v, 0.0) + jnp.log1p(jnp.exp(-jnp.abs(v)))


def _const(shape):
    return pl.BlockSpec(shape, lambda i: (0,) * len(shape), pipeline_mode=pl.Buffered(1))


def _params(mb, **kw):
    return pltpu.CompilerParams(dimension_semantics=('arbitrary',), vmem_limit_bytes=mb * 1024 * 1024, **kw)


def _cost(flops, nbytes):
    return pl.CostEstimate(flops=int(flops), bytes_accessed=int(nbytes), transcendentals=0)


def _taps(x_ref, halo_ref, r):
    cur = x_ref[pl.ds(pl.multiple_of(r * Q, Q), Q), :].astype(F32)
    at = pl.multiple_of(jnp.maximum(r * Q - 16, 0), 16)
    prev = jnp.where(r == 0, halo_ref[...], x_ref[pl.ds(at, 16), :]).astype(F32)
    ext = jnp.concatenate([prev, cur], 0)
    return [cur] + [pltpu.roll(ext, k, 0)[16:] for k in range(1, KCONV)]


def _conv_fwd_kernel(x_ref, halo_ref, w_ref, b_ref, o_ref):
    nr = x_ref.shape[0] // Q

    def body(r, _):
        taps = _taps(x_ref, halo_ref, r)
        u = b_ref[...] + sum(w_ref[k:k + 1, :] * taps[k] for k in range(KCONV))
        o_ref[pl.ds(pl.multiple_of(r * Q, Q), Q), :] = (u * jax.nn.sigmoid(u)).astype(BF16)
        return 0

    lax.fori_loop(0, nr, body, 0)


def _conv_fwd(xb, halo, w, b, cw=256):
    t = xb.shape[0]
    return pl.pallas_call(
        _conv_fwd_kernel,
        grid=(CD // cw,),
        in_specs=[pl.BlockSpec((t, cw), lambda i: (0, i)), pl.BlockSpec((16, cw), lambda i: (0, i)),
                  pl.BlockSpec((KCONV, cw), lambda i: (0, i)), pl.BlockSpec((1, cw), lambda i: (0, i))],
        out_specs=pl.BlockSpec((t, cw), lambda i: (0, i)),
        out_shape=jax.ShapeDtypeStruct((t, CD), BF16),
        compiler_params=_params(40),
        cost_estimate=_cost(25e9, 4 * t * CD),
        name='conv_fwd',
    )(xb, halo, w, b)


def _conv_bwd_kernel(x_ref, halo_ref, d_ref, w_ref, b_ref, o_ref, gw_ref, gb_ref, head_ref, tail_ref, nxt):
    nr = x_ref.shape[0] // Q
    cw = x_ref.shape[1]
    gw_ref[...] = jnp.zeros_like(gw_ref)
    gb_ref[...] = jnp.zeros_like(gb_ref)
    nxt[...] = jnp.zeros_like(nxt)

    def fold(v):
        return jnp.sum(v.reshape(Q // 8, 8, cw), 0)

    def body(k, _):
        r = nr - 1 - k
        taps = _taps(x_ref, halo_ref, r)
        u = b_ref[...] + sum(w_ref[i:i + 1, :] * taps[i] for i in range(KCONV))
        sg = jax.nn.sigmoid(u)
        rows = pl.ds(pl.multiple_of(r * Q, Q), Q)
        du = d_ref[rows, :].astype(F32) * (sg * (1.0 + u * (1.0 - sg)))
        gb_ref[...] += fold(du)
        for i in range(KCONV):
            gw_ref[8 * i:8 * i + 8, :] += fold(du * taps[i])
        ext = jnp.concatenate([du, nxt[...]], 0)
        dx = w_ref[0:1, :] * du + sum(
            w_ref[i:i + 1, :] * pltpu.roll(ext, Q + 8 - i, 0)[:Q] for i in range(1, KCONV))
        nxt[...] = du[:8]
        o_ref[rows, :] = dx.astype(BF16)

        @pl.when(k == 0)
        def _():
            tail_ref[...] = dx[Q - 16:]

        return 0

    lax.fori_loop(0, nr, body, 0)
    head_ref[...] = nxt[...]


def _conv_bwd(xb, halo, dxc, w, b, cw=256):
    t = xb.shape[0]
    col = lambda r: pl.BlockSpec((r, cw), lambda i: (0, i))
    return pl.pallas_call(
        _conv_bwd_kernel,
        grid=(CD // cw,),
        in_specs=[col(t), col(16), col(t), col(KCONV), col(1)],
        out_specs=[col(t), col(8 * KCONV), col(8), col(8), col(16)],
        out_shape=[jax.ShapeDtypeStruct((t, PX), BF16), jax.ShapeDtypeStruct((8 * KCONV, CD), F32),
                   jax.ShapeDtypeStruct((8, CD), F32), jax.ShapeDtypeStruct((8, CD), F32),
                   jax.ShapeDtypeStruct((16, CD), F32)],
        scratch_shapes=[pltpu.VMEM((8, cw), F32)],
        compiler_params=_params(40),
        cost_estimate=_cost(50e9, 6 * t * CD),
        name='conv_bwd',
    )(xb, halo, dxc, w, b)


def _state_kernel(xc_ref, dtr_ref, bias_ref, al_ref, e_ref, cd_ref, cdt_ref, hst_ref, h_ref, s_ref):
    i = pl.program_id(0)

    @pl.when(i == 0)
    def _():
        h_ref[...] = jnp.zeros_like(h_ref)
        s_ref[...] = jnp.zeros_like(s_ref)

    dt = _softplus(dtr_ref[...].astype(F32) + bias_ref[...])
    a = -jnp.exp(al_ref[...]) * dt
    tri = (_iota((Q, Q), 0) >= _iota((Q, Q), 1)).astype(F32)
    c = lax.dot_general(tri, a, (((1,), (0,)), ((), ())), precision=HI, preferred_element_type=F32)
    s_ref[...] += jnp.broadcast_to(c[Q - 1:Q], s_ref.shape)
    c2 = c * LOG2E
    cd = jnp.concatenate([c2, dt], 1)
    cd_ref[...] = cd
    cdt_ref[...] = cd.T
    f3 = _split3(dt * jnp.exp2(c2[Q - 1:Q] - c2))
    ea3 = _split3(jnp.exp2(c2[Q - 16:]))
    bt = xc_ref[:, E:E + N].astype(F32).T.astype(BF16)

    def body(j, _):
        L = _lanes(j, 256)
        ej = e_ref[:, L]
        xw = (xc_ref[:, L].astype(F32) * _dot(f3, ej)).astype(BF16)
        st = _dot(bt, xw)
        h = h_ref[:, L]
        hst_ref[:, L] = h
        h_ref[:, L] = h * _dot(ea3, ej)[15:16] + st
        return 0

    lax.fori_loop(0, E // 256, body, 0)


def _states(xc, dtr, bias, al, e64):
    t = xc.shape[0]
    nc = t // Q
    row = lambda w: pl.BlockSpec((Q, w), lambda i: (i, 0))
    return pl.pallas_call(
        _state_kernel,
        grid=(nc,),
        in_specs=[row(CD), row(H), _const((1, H)), _const((1, H)), _const((256, E))],
        out_specs=[row(2 * H), pl.BlockSpec((None, 2 * H, Q), lambda i: (i, 0, 0)),
                   pl.BlockSpec((None, N, E), lambda i: (i, 0, 0)), pl.BlockSpec((N, E), lambda i: (0, 0)),
                   pl.BlockSpec((8, H), lambda i: (0, 0))],
        out_shape=[jax.ShapeDtypeStruct((t, 2 * H), F32), jax.ShapeDtypeStruct((nc, 2 * H, Q), F32),
                   jax.ShapeDtypeStruct((nc, N, E), F32), jax.ShapeDtypeStruct((N, E), F32),
                   jax.ShapeDtypeStruct((8, H), F32)],
        compiler_params=_params(48),
        cost_estimate=_cost(25e9, 70e6),
        name='states',
    )(xc, dtr, bias, al, e64)


def _fwd_kernel(xc_ref, cd_ref, cdt_ref, hst_ref, hin_ref, z_ref, dyn_ref, d_ref, nw_ref, e_ref, e2_ref,
                yn_ref, dz_ref, dy_ref, hs_ref, dh_ref, gl_ref, row_ref, dnw_ref, dd_ref,
                y_s, sc_s, xm_s, cb_s, ece, acc1, acc2, p_hi, p_lo, q_s):
    i = pl.program_id(0)

    @pl.when(i == 0)
    def _():
        sc_s[...] = jnp.zeros_like(sc_s)
        ece[...] = jnp.ones_like(ece)
        gl_ref[...] = jnp.zeros_like(gl_ref)
        dnw_ref[...] = jnp.zeros_like(dnw_ref)
        dd_ref[...] = jnp.zeros_like(dd_ref)

    c2 = cd_ref[:, :H]
    c3 = _split3(c2)
    ec3 = _split3(jnp.exp2(c2))
    bm = xc_ref[:, E:E + N]
    cm = xc_ref[:, E + N:]
    ct = cm.astype(F32).T.astype(BF16)
    causal = _iota((Q, Q), 0) >= _iota((Q, Q), 1)
    cb_s[...] = jnp.where(causal, _nt(cm, bm), 0.0)
    acc1[...] = jnp.zeros_like(acc1)
    acc2[...] = jnp.zeros_like(acc2)
    head = _iota((1, 256), 1) // 64

    def quad(j, _):
        L = _lanes(j, 256)
        ej = e_ref[:, L]
        xq = xc_ref[:, L]
        ccol = _dot(c3, e2_ref[:, _lanes(j, 512)])
        h = hst_ref[:, L] + ece[0:1, L] * hin_ref[:, L]
        hs_ref[:, L] = h
        yi = _dot(cm, h.astype(BF16)) * _dot(ec3, ej)
        for k in range(4):
            crow = cdt_ref[pl.ds(4 * j + k, 1), :]
            drow = cdt_ref[pl.ds(H + 4 * j + k, 1), :]
            cc = ccol[:, k * 128:k * 128 + 128]
            for (a, b) in ((0, 0), (1, 0), (1, 1)):
                ra, rb = slice(a * HB, a * HB + HB), slice(b * HB, b * HB + HB)
                seg = jnp.minimum(cc[ra] - crow[:, rb], 0.0)
                w = jnp.exp2(seg) * drow[:, rb]
                sc_s[ra, k * Q + b * HB:k * Q + b * HB + HB] = (cb_s[ra, rb] * w).astype(BF16)
            xm_s[k * Q:k * Q + Q, :] = jnp.where(head == k, xq, jnp.zeros_like(xq))
        y = yi + _dot(sc_s[...], xm_s[...])
        y_s[:, L] = y
        z = z_ref[:, L].astype(F32)
        g = (y + d_ref[:, L] * xq.astype(F32)) * (z * jax.nn.sigmoid(z))
        gg = g * g
        gd = g * (dyn_ref[:, L].astype(F32) * nw_ref[:, L])
        acc1[...] += gg[:, :128] + gg[:, 128:]
        acc2[...] += gd[:, :128] + gd[:, 128:]
        return 0

    lax.fori_loop(0, E // 256, quad, 0)
    r = lax.rsqrt(jnp.sum(acc1[...], 1, keepdims=True) / E + EPS)
    m = jnp.sum(acc2[...], 1, keepdims=True) / E * (r * r * r)
    acc1[...] = jnp.broadcast_to(r, acc1.shape)
    acc2[...] = jnp.broadcast_to(m, acc2.shape)
    row_ref[...] = jnp.zeros_like(row_ref)
    RB = 64

    def gate(j, _):
        L = _lanes(j, 256)
        ej = e_ref[:, L]
        ecq = _dot(ec3, ej)
        q_s[...] = ecq

        def rows(k, _):
            R = pl.ds(pl.multiple_of(k * RB, RB), RB)
            x = xc_ref[R, L].astype(F32)
            ys = y_s[R, L]
            y = ys + d_ref[:, L] * x
            z = z_ref[R, L].astype(F32)
            sg = jax.nn.sigmoid(z)
            sz = z * sg
            g = y * sz
            rb = jnp.concatenate([acc1[R, :], acc1[R, :]], 1)
            mb = jnp.concatenate([acc2[R, :], acc2[R, :]], 1)
            gr = g * rb
            dn = dyn_ref[R, L].astype(F32)
            nw = nw_ref[:, L]
            yn_ref[R, L] = (gr * nw).astype(BF16)
            dnw_ref[:, L] += jnp.sum((dn * gr).reshape(RB // 8, 8, 256), 0)
            dg = rb * (dn * nw) - g * mb
            dy = dg * sz
            dz_ref[R, L] = (dg * y * (sg + sz * (1.0 - sg))).astype(BF16)
            dy_ref[R, L] = dy
            dd_ref[:, L] += jnp.sum((dy * x).reshape(RB // 8, 8, 256), 0)
            hi, lo = _split2(dy.astype(BF16).astype(F32) * ys)
            p_hi[R, :] = hi
            p_lo[R, :] = lo
            q_s[R, :] = q_s[R, :] * dy
            return 0

        lax.fori_loop(0, Q // RB, rows, 0)
        er = e_ref[0:2 * H, L]
        row_ref[...] += _nt(p_hi[...], er) + _nt(p_lo[...], er)
        dh = _dot(ct, q_s[...].astype(BF16)).astype(BF16)
        dh_ref[:, L] = dh
        gl_ref[:, L] += ece[0:1, L] * dh.astype(F32)
        ece[:, L] = ece[:, L] * ecq[Q - 1:Q]
        return 0

    lax.fori_loop(0, E // 256, gate, 0)


def _fwd(xc, cd, cdt, hst, hin, z, dyn, dx, nw, e64, e128):
    t = xc.shape[0]
    nc = t // Q
    row = lambda w: pl.BlockSpec((Q, w), lambda i: (i, 0))
    blk = lambda a, b: pl.BlockSpec((None, a, b), lambda i: (i, 0, 0))
    fix = lambda a, b: pl.BlockSpec((a, b), lambda i: (0, 0))
    return pl.pallas_call(
        _fwd_kernel,
        grid=(nc,),
        in_specs=[row(CD), row(2 * H), blk(2 * H, Q), blk(N, E), _const((N, E)), row(E), row(E), _const((1, E)),
                  _const((1, E)), _const((256, E)), _const((256, 2 * E))],
        out_specs=[row(E), row(E), row(E), blk(N, E), blk(N, E), fix(N, E), row(2 * H), fix(8, E), fix(8, E)],
        out_shape=[jax.ShapeDtypeStruct((t, E), BF16), jax.ShapeDtypeStruct((t, E), BF16),
                   jax.ShapeDtypeStruct((t, E), F32), jax.ShapeDtypeStruct((nc, N, E), F32),
                   jax.ShapeDtypeStruct((nc, N, E), BF16), jax.ShapeDtypeStruct((N, E), F32),
                   jax.ShapeDtypeStruct((t, 2 * H), F32), jax.ShapeDtypeStruct((8, E), F32),
                   jax.ShapeDtypeStruct((8, E), F32)],
        scratch_shapes=[pltpu.VMEM((Q, E), F32), pltpu.VMEM((Q, 4 * Q), BF16), pltpu.VMEM((4 * Q, 256), BF16),
                        pltpu.VMEM((Q, Q), F32), pltpu.VMEM((8, E), F32), pltpu.VMEM((Q, 128), F32),
                        pltpu.VMEM((Q, 128), F32), pltpu.VMEM((Q, 256), BF16), pltpu.VMEM((Q, 256), BF16),
                        pltpu.VMEM((Q, 256), F32)],
        compiler_params=_params(60),
        cost_estimate=_cost(150e9, 270e6),
        name='ssd_fwd_gate',
    )(xc, cd, cdt, hst, hin, z, dyn, dx, nw, e64, e128)


def _bwd_kernel(xc_ref, cd_ref, cdt_ref, hs_ref, dh_ref, gin_ref, dae_ref, dy_ref, row_ref, d_ref, dtr_ref, bias_ref,
                al_ref, e_ref, e2_ref,
                dxc_ref, ddtr_ref, red_ref,
                g_s, sc_s, xm_s, dm_s, cb_s, w_s, dcb_s, dae_s, col_s, db_s, dc_s):
    i = pl.program_id(0)

    @pl.when(i == 0)
    def _():
        sc_s[...] = jnp.zeros_like(sc_s)
        g_s[...] = gin_ref[...]
        dae_s[...] = dae_ref[...]
        red_ref[...] = jnp.zeros_like(red_ref)

    c2 = cd_ref[:, :H]
    dt = cd_ref[:, H:]
    c3 = _split3(c2)
    d3 = _split3(dt)
    ec3 = _split3(jnp.exp2(c2))
    f3 = _split3(dt * jnp.exp2(c2[Q - 1:Q] - c2))
    bm = xc_ref[:, E:E + N]
    cm = xc_ref[:, E + N:]
    causal = _iota((Q, Q), 0) <= _iota((Q, Q), 1)
    cb_s[...] = jnp.where(causal, _nt(bm, cm), 0.0)
    dcb_s[...] = jnp.zeros_like(dcb_s)
    col_s[...] = jnp.zeros_like(col_s)
    db_s[...] = jnp.zeros_like(db_s)
    dc_s[...] = jnp.zeros_like(dc_s)
    head = _iota((1, 256), 1) // 64
    er0 = e_ref[0:2 * H, :]
    dae = dae_s[...]
    dhi = dae.astype(BF16)
    dmid = (dae - dhi.astype(F32)).astype(BF16)
    dlo = (dae - dhi.astype(F32) - dmid.astype(F32)).astype(BF16)
    dae_h = (_nt(dhi, er0) + _nt(dmid, er0) + _nt(dlo, er0))[0:1, :H]

    def quad(j, _):
        L = _lanes(j, 256)
        ej = e_ref[:, L]
        xq = xc_ref[:, L]
        dy = dy_ref[:, L]
        dyb = dy.astype(BF16)
        for k in range(4):
            sel = head == k
            xm_s[k * Q:k * Q + Q, :] = jnp.where(sel, xq, jnp.zeros_like(xq))
            dm_s[k * Q:k * Q + Q, :] = jnp.where(sel, dyb, jnp.zeros_like(dyb))
        e2j = e2_ref[:, _lanes(j, 512)]
        ccol = _dot(c3, e2j)
        dcol = _dot(d3, e2j)
        w_s[...] = _nt(xm_s[...], dyb)
        for k in range(4):
            crow = cdt_ref[pl.ds(4 * j + k, 1), :]
            cc = ccol[:, k * 128:k * 128 + 128]
            dc = dcol[:, k * 128:k * 128 + 128]
            for (a, b) in ((0, 0), (0, 1), (1, 1)):
                ra, rb = slice(a * HB, a * HB + HB), slice(b * HB, b * HB + HB)
                seg = jnp.minimum(crow[:, rb] - cc[ra], 0.0)
                w = jnp.exp2(seg) * dc[ra]
                sc_s[ra, k * Q + b * HB:k * Q + b * HB + HB] = (cb_s[ra, rb] * w).astype(BF16)
                ds = w_s[k * Q + a * HB:k * Q + a * HB + HB, rb].astype(BF16).astype(F32)
                dcb_s[ra, rb] += ds * w
        dxs = _dot(sc_s[...], dm_s[...])
        fq = _dot(f3, ej)
        g = g_s[:, L]
        gb = g.astype(BF16)
        x = xq.astype(F32)
        dxw = _dot(bm, gb).astype(BF16).astype(F32)
        dxs = dxs + fq * dxw
        db_s[...] += _nt((x * fq).astype(BF16), gb)
        ecq = _dot(ec3, ej)
        hs = hs_ref[:, L]
        dc_s[...] += _nt((ecq * dy).astype(BF16), hs.astype(BF16))
        hi, lo = _split2(x * dxs)
        er = e_ref[0:2 * H, L]
        col_s[...] += _nt(hi, er) + _nt(lo, er)
        dxc_ref[:, L] = (dxs + d_ref[:, L] * dy).astype(BF16)
        gn = g * ecq[Q - 1:Q] + dh_ref[:, L].astype(F32)
        g_s[:, L] = gn
        dae_s[:, L] = jnp.broadcast_to(jnp.sum(gn * hs, 0, keepdims=True), (8, 256))
        return 0

    lax.fori_loop(0, E // 256, quad, 0)
    dcb = jnp.where(causal, dcb_s[...], 0.0)
    dxc_ref[:, E:E + N] = (db_s[...] + _dot(dcb.astype(BF16), cm)).astype(BF16)
    dxc_ref[:, E + N:] = (dc_s[...] + _dot(dcb.T.astype(BF16), bm)).astype(BF16)

    col = col_s[:, :H]
    dcs = row_ref[:, :H] - col
    dcs = dcs + jnp.where(_iota((Q, H), 0) == Q - 1, dae_h, 0.0)
    triu = (_iota((Q, Q), 0) <= _iota((Q, Q), 1)).astype(F32)
    da = lax.dot_general(triu, dcs, (((1,), (0,)), ((), ())), precision=HI, preferred_element_type=F32)
    na = -jnp.exp(al_ref[...])
    ddt = jnp.where(dt > 0.0, col / jnp.where(dt > 0.0, dt, 1.0), 0.0) + da * na
    ddtr = ddt * jax.nn.sigmoid(dtr_ref[...].astype(F32) + bias_ref[...])
    ddtr_ref[...] = ddtr.astype(BF16)
    both = jnp.concatenate([ddtr, da * (na * dt)], 1)
    red_ref[...] += jnp.sum(both.reshape(Q // 8, 8, 2 * H), 0)


def _bwd(xc, cd, cdt, hs, dh, gin, dae, dy, row, dx, dtr, bias, al, e64, e128):
    t = xc.shape[0]
    nc = t // Q
    rows = lambda w: pl.BlockSpec((Q, w), lambda i: (nc - 1 - i, 0))
    blk = lambda a, b: pl.BlockSpec((None, a, b), lambda i: (nc - 1 - i, 0, 0))
    fix = lambda a, b: pl.BlockSpec((a, b), lambda i: (0, 0))
    return pl.pallas_call(
        _bwd_kernel,
        grid=(nc,),
        in_specs=[rows(CD), rows(2 * H), blk(2 * H, Q), blk(N, E), blk(N, E), _const((N, E)), _const((8, E)), rows(E),
                  rows(2 * H), _const((1, E)), rows(H), _const((1, H)), _const((1, H)), _const((256, E)),
                  _const((256, 2 * E))],
        out_specs=[rows(CD), rows(H), fix(8, 2 * H)],
        out_shape=[jax.ShapeDtypeStruct((t, CD), BF16), jax.ShapeDtypeStruct((t, H), BF16),
                   jax.ShapeDtypeStruct((8, 2 * H), F32)],
        scratch_shapes=[pltpu.VMEM((N, E), F32), pltpu.VMEM((Q, 4 * Q), BF16), pltpu.VMEM((4 * Q, 256), BF16),
                        pltpu.VMEM((4 * Q, 256), BF16), pltpu.VMEM((Q, Q), F32), pltpu.VMEM((4 * Q, Q), F32),
                        pltpu.VMEM((Q, Q), F32), pltpu.VMEM((8, E), F32), pltpu.VMEM((Q, 2 * H), F32),
                        pltpu.VMEM((Q, N), F32), pltpu.VMEM((Q, N), F32)],
        compiler_params=_params(60),
        cost_estimate=_cost(150e9, 220e6),
        name='ssd_bwd',
    )(xc, cd, cdt, hs, dh, gin, dae, dy, row, dx, dtr, bias, al, e64, e128)


def _prefix(s):
    k = s.shape[0]
    cs = jnp.cumsum(s, 0)
    diff = (cs - s)[:, None] - cs[None, :]
    m = (jnp.arange(k)[:, None] > jnp.arange(k)[None, :]).reshape((k, k) + (1,) * (s.ndim - 1))
    return jnp.where(m, jnp.exp(jnp.where(m, diff, 0.0)), 0.0)


def _wide(v):
    return jnp.repeat(v, E // H, axis=-1)


def solution(mesh):
    nseq = mesh.shape['seq']
    fwd = [(i, i + 1) for i in range(nseq - 1)]
    bwd = [(i + 1, i) for i in range(nseq - 1)]
    core = [(i, i ^ 1) for i in range(nseq)]
    chip = [(i, i ^ 2) for i in range(nseq)]

    def local(x, dout, W_in, conv_w, conv_b, dt_bias, A_log, D_skip, norm_w, W_out):
        t, dm = x.shape
        idx = lax.axis_index('seq')
        c, k = idx % 2, idx // 2
        rows = jnp.arange(256)
        lane = jnp.arange(2 * E)
        e128 = ((rows[:, None] % H == lane[None, :] // 128) & (rows[:, None] < 3 * H)).astype(BF16)
        e64 = ((rows[:, None] % H == lane[None, :E] // 64) & (rows[:, None] < 3 * H)).astype(BF16)
        bias, al = dt_bias[None], A_log[None]
        dwide = _wide(D_skip)[None]
        Wz, Wx = W_in[:, :E], W_in[:, E:]

        xb = jnp.dot(x, Wx, preferred_element_type=F32).astype(BF16)
        halo = lax.ppermute(xb[t - 16:], 'seq', fwd)
        dtr = xb[:, CD:]
        xc = _conv_fwd(xb, halo, conv_w, conv_b[None])
        cd, cdt, hst, h_loc, s8 = _states(xc, dtr, bias, al, e64)
        s = s8[0]
        s_all = lax.all_gather(s, 'seq')
        h_all = lax.all_gather(h_loc, 'seq')
        wd = _wide(_prefix(s_all))
        h_in = jnp.sum(wd[idx][:, None, :] * h_all, 0)
        h_fin = h_loc + _wide(jnp.exp(s))[None] * h_in
        z = jnp.dot(x, Wz, preferred_element_type=F32).astype(BF16)
        dyn = _nt(dout, W_out).astype(BF16)
        yn, dz, dy, hs, dh, g_loc, row, dnw8, dd8 = _fwd(xc, cd, cdt, hst, h_in, z, dyn, dwide, norm_w[None], e64, e128)
        g_all = lax.all_gather(g_loc, 'seq')

        def quarters(a):
            w = a.shape[1] // 4
            cut = lambda cc, kk: lax.dynamic_slice_in_dim(a, (2 * cc + kk) * w, w, 1)
            return (jnp.concatenate([cut(1 - c, 1 - k), cut(1 - c, k)], 1), cut(c, 1 - k), cut(c, k))

        xs, ds = quarters(x), quarters(dout)

        def spread(mine):
            other = lax.ppermute(mine, 'seq', chip)
            mine_p = lax.ppermute(mine, 'seq', core)
            other_p = lax.ppermute(other, 'seq', core)
            return [(2 * c + k, mine), (2 * c + 1 - k, other), (2 - 2 * c + k, mine_p), (3 - 2 * c - k, other_p)]

        sO = _tn(yn, ds[0])
        rO = lax.ppermute(sO, 'seq', core)
        sZ = _tn(xs[0], dz)
        rZ = lax.ppermute(sZ, 'seq', core)
        dh_fin = jnp.sum(wd[:, idx][:, None, :] * g_all, 0)
        dae = jnp.broadcast_to(jnp.sum(dh_fin * h_fin, 0)[None], (8, E))
        w4 = dm // 4
        fO = _tn(yn, ds[1]) + rO[:, :w4]
        fZ = _tn(xs[1], dz) + rZ[:w4]
        fO, fZ, dy, dae = lax.optimization_barrier((fO, fZ, dy, dae))
        gO = lax.ppermute(fO, 'seq', chip)
        gZ = lax.ppermute(fZ, 'seq', chip)
        oO = _tn(yn, ds[2]) + rO[:, w4:]
        oZ = _tn(xs[2], dz) + rZ[w4:]
        dxc, ddtr, red = _bwd(xc, cd, cdt, hs, dh, dh_fin, dae, dy, row, dwide, dtr, bias, al, e64, e128)
        dxc, gO, gZ, oO, oZ = lax.optimization_barrier((dxc, gO, gZ, oO, oZ))
        pO = spread((oO + gO).astype(BF16))
        pZ = spread((oZ + gZ).astype(BF16))
        dxb, gw8, gb8, head, tail = _conv_bwd(xb, halo, dxc, conv_w, conv_b[None])
        nxt = lax.ppermute(head, 'seq', bwd)
        fix = sum(conv_w[j] * jnp.pad(nxt[:j], ((16 - j, 0), (0, 0))) for j in range(1, KCONV))
        dxb = lax.dynamic_update_slice(dxb, (tail + fix).astype(BF16), (t - 16, 0))
        dxb = lax.dynamic_update_slice(dxb, ddtr, (0, CD))

        dcw = jnp.sum(gw8.reshape(KCONV, 8, CD), 1)
        small = jnp.concatenate([dcw.reshape(-1), jnp.sum(gb8, 0), jnp.sum(red, 0), jnp.sum(dd8, 0).reshape(H, E // H).sum(1),
                                 jnp.sum(dnw8, 0)])
        small = small + lax.ppermute(small, 'seq', core)
        small = small + lax.ppermute(small, 'seq', chip)

        sX = _tn(xs[0], dxb)
        rX = lax.ppermute(sX, 'seq', core)
        fX = _tn(xs[1], dxb) + rX[:w4]
        fX, small = lax.optimization_barrier((fX, small))
        gX = lax.ppermute(fX, 'seq', chip)
        oX = _tn(xs[2], dxb) + rX[w4:]
        dx0 = _nt(dz, Wz)
        pX = spread((oX + gX).astype(BF16))
        dx = (dx0 + _nt(dxb, Wx)).astype(BF16)

        def place(out, pieces, axis, col=0):
            for pos, p in pieces:
                w = p.shape[axis]
                at = (pos * w, jnp.int32(col)) if axis == 0 else (jnp.int32(0), pos * w)
                out = lax.dynamic_update_slice(out, p, at)
            return out

        dW_in = place(place(jnp.zeros((dm, E + PX), BF16), pZ, 0), pX, 0, E)
        dW_out = place(jnp.zeros((E, dm), BF16), pO, 1)
        cuts = []
        for n in (KCONV * CD, CD, H, H, H, E):
            cuts.append(small[:n])
            small = small[n:]
        dcw, dcb, ddtb, dal, dD, dnw = cuts
        dcw = dcw.reshape(KCONV, CD)
        return dx, dW_in, dcw, dcb, ddtb, dal, dD, dnw, dW_out

    xs = P(('data', 'seq'), None)
    return jax.shard_map(local, mesh=mesh, in_specs=(xs, xs) + (P(),) * 8,
                         out_specs=(xs, P('data', None), P('data', None), P('data'), P('data'), P('data'),
                                    P('data'), P('data'), P('data', None)),
                         check_vma=False)
```

```python
import jax
import jax.numpy as jnp
from jax import lax
from jax.experimental import pallas as pl
from jax.experimental.pallas import tpu as pltpu
from jax.sharding import PartitionSpec as P

Q = 256
N = 128
H = 64
E = 4096
CD = E + 2 * N
PX = CD + H
KCONV = 4
EPS = 1e-5
LOG2E = 1.4426950408889634
F32 = jnp.float32
BF16 = jnp.bfloat16
HB = 128
R8 = 8
R16 = 16


def _dot(a, b):
    return lax.dot_general(a, b, (((1,), (0,)), ((), ())), preferred_element_type=F32)


def _tn(a, b):
    return lax.dot_general(a, b, (((0,), (0,)), ((), ())), preferred_element_type=F32)


def _nt(a, b):
    return lax.dot_general(a, b, (((1,), (1,)), ((), ())), preferred_element_type=F32)


def _twice(body, a, b):
    def step(j, _):
        body(2 * j, *a)
        body(2 * j + 1, *b)
        return 0

    lax.fori_loop(0, E // 512, step, 0)


def _lanes(j, w):
    return pl.ds(pl.multiple_of(j * w, w), w)


def _iota(shape, d):
    return lax.broadcasted_iota(jnp.int32, shape, d)


def _split3(v):
    hi = v.astype(BF16).astype(F32)
    mid = (v - hi).astype(BF16).astype(F32)
    lo = v - hi - mid
    return jnp.concatenate([hi, mid, lo, jnp.zeros_like(v)], 1).astype(BF16)


def _sum3(v):
    return v[:, :H] + v[:, H:2 * H] + v[:, 2 * H:3 * H]


def _split2(v):
    hi = v.astype(BF16)
    return hi, (v - hi.astype(F32)).astype(BF16)


def _softplus(v):
    return jnp.maximum(v, 0.0) + jnp.log1p(jnp.exp(-jnp.abs(v)))


def _const(shape):
    return pl.BlockSpec(shape, lambda i: (0,) * len(shape), pipeline_mode=pl.Buffered(1))


def _params(mb, **kw):
    return pltpu.CompilerParams(dimension_semantics=('arbitrary',), vmem_limit_bytes=mb * 1024 * 1024, **kw)


def _cost(flops, nbytes):
    return pl.CostEstimate(flops=int(flops), bytes_accessed=int(nbytes), transcendentals=0)


def _load_taps(x_ref, halo_ref, scr, r, h):
    hl = slice(h * N, h * N + N)
    at = pl.multiple_of(jnp.maximum(r * Q - R16, 0), R16)
    scr[0:R16, :] = jnp.where(r == 0, halo_ref[:, hl], x_ref[pl.ds(at, R16), hl]).astype(F32)
    scr[R16:, :] = x_ref[pl.ds(pl.multiple_of(r * Q, Q), Q), hl].astype(F32)


def _conv_fwd_kernel(x_ref, halo_ref, w_ref, b_ref, o_ref, *scrs):
    nr = x_ref.shape[0] // Q

    def body(r, _):
        for h, scr in enumerate(scrs):
            hl = slice(h * N, h * N + N)
            _load_taps(x_ref, halo_ref, scr, r, h)
            u = b_ref[:, hl] + sum(w_ref[k:k + 1, hl] * scr[R16 - k:R16 - k + Q, :] for k in range(KCONV))
            o_ref[pl.ds(pl.multiple_of(r * Q, Q), Q), hl] = (u * jax.nn.sigmoid(u)).astype(BF16)
        return 0

    lax.fori_loop(0, nr, body, 0)


def _conv_fwd(xb, halo, w, b, cw=Q):
    t = xb.shape[0]
    return pl.pallas_call(
        _conv_fwd_kernel,
        grid=(CD // cw,),
        in_specs=[pl.BlockSpec((t, cw), lambda i: (0, i)), pl.BlockSpec((R16, cw), lambda i: (0, i)),
                  pl.BlockSpec((KCONV, cw), lambda i: (0, i)), pl.BlockSpec((1, cw), lambda i: (0, i))],
        out_specs=pl.BlockSpec((t, cw), lambda i: (0, i)),
        out_shape=jax.ShapeDtypeStruct((t, CD), BF16),
        scratch_shapes=[pltpu.VMEM((Q + R16, N), F32)] * (cw // N),
        compiler_params=_params(40),
        cost_estimate=_cost(25e9, 4 * t * CD),
        name='conv_fwd',
    )(xb, halo, w, b)


def _conv_bwd_kernel(x_ref, halo_ref, d_ref, w_ref, b_ref, o_ref, gw_ref, gb_ref, tail_ref, *scrs):
    nr = x_ref.shape[0] // Q
    nh = x_ref.shape[1] // N
    xscr, dscr = scrs[:nh], scrs[nh:]
    gw_ref[...] = jnp.zeros_like(gw_ref)
    gb_ref[...] = jnp.zeros_like(gb_ref)
    for d in dscr:
        d[0:R8, :] = jnp.zeros((R8, N), F32)

    def fold(v):
        return jnp.sum(v.reshape(Q // R8, R8, N), 0)

    def body(k, _):
        r = nr - 1 - k
        rows = pl.ds(pl.multiple_of(r * Q, Q), Q)
        for h in range(nh):
            hl = slice(h * N, h * N + N)
            scr, d = xscr[h], dscr[h]
            _load_taps(x_ref, halo_ref, scr, r, h)
            u = b_ref[:, hl] + sum(w_ref[i:i + 1, hl] * scr[R16 - i:R16 - i + Q, :] for i in range(KCONV))
            sg = jax.nn.sigmoid(u)
            du = d_ref[rows, hl].astype(F32) * (sg * (1.0 + u * (1.0 - sg)))
            d[Q:, :] = d[0:R8, :]
            d[0:Q, :] = du
            gb_ref[:, hl] += fold(du)
            for i in range(KCONV):
                gw_ref[R8 * i:R8 * i + R8, hl] += fold(du * scr[R16 - i:R16 - i + Q, :])
            dx = sum(w_ref[i:i + 1, hl] * d[i:i + Q, :] for i in range(KCONV))
            o_ref[rows, hl] = dx.astype(BF16)

            @pl.when(k == 0)
            def _():
                tail_ref[:, hl] = dx[Q - R16:]

        return 0

    lax.fori_loop(0, nr, body, 0)


def _conv_bwd(xb, halo, dxc, w, b, cw=Q):
    t = xb.shape[0]
    col = lambda r: pl.BlockSpec((r, cw), lambda i: (0, i))
    return pl.pallas_call(
        _conv_bwd_kernel,
        grid=(CD // cw,),
        in_specs=[col(t), col(R16), col(t), col(KCONV), col(1)],
        out_specs=[col(t), col(R8 * KCONV), col(R8), col(R16)],
        out_shape=[jax.ShapeDtypeStruct((t, PX), BF16), jax.ShapeDtypeStruct((R8 * KCONV, CD), F32),
                   jax.ShapeDtypeStruct((R8, CD), F32), jax.ShapeDtypeStruct((R16, CD), F32)],
        scratch_shapes=[pltpu.VMEM((Q + R16, N), F32)] * (cw // N) + [pltpu.VMEM((Q + R8, N), F32)] * (cw // N),
        compiler_params=_params(40),
        cost_estimate=_cost(50e9, 6 * t * CD),
        name='conv_bwd',
    )(xb, halo, dxc, w, b)


def _state_kernel(xc_ref, dtr_ref, bias_ref, al_ref, e_ref, cd_ref, cdt_ref, c3_ref, d3_ref, ec3_ref, f3_ref, hst_ref, h_ref,
                  s_ref, fe_s):
    i = pl.program_id(0)

    @pl.when(i == 0)
    def _():
        h_ref[...] = jnp.zeros_like(h_ref)
        s_ref[...] = jnp.zeros_like(s_ref)

    dt = _softplus(dtr_ref[...].astype(F32) + bias_ref[...])
    a = -jnp.exp(al_ref[...]) * dt
    tri = (_iota((Q, Q), 0) >= _iota((Q, Q), 1)).astype(BF16)
    c = _sum3(_dot(tri, _split3(a)))
    s_ref[...] += jnp.broadcast_to(c[Q - 1:Q], s_ref.shape)
    c2 = c * LOG2E
    cd = jnp.concatenate([c2, dt], 1)
    cd_ref[...] = cd
    cdt_ref[...] = cd.T
    c3_ref[...] = _split3(c2)
    d3_ref[...] = _split3(dt)
    ec3 = _split3(jnp.exp2(c2))
    ec3_ref[...] = ec3
    f3 = _split3(dt * jnp.exp2(c2[Q - 1:Q] - c2))
    f3_ref[...] = f3
    fe_s[0:Q, :] = f3
    fe_s[Q:, :] = ec3[Q - R16:]
    bt = xc_ref[:, E:E + N].astype(F32).T.astype(BF16)

    def body(j, _):
        L = _lanes(j, 512)
        fe = _dot(fe_s[...], e_ref[:, L])
        xw = (xc_ref[:, L].astype(F32) * fe[:Q]).astype(BF16)
        st = _dot(bt, xw)
        h = h_ref[:, L]
        hst_ref[:, L] = h
        h_ref[:, L] = h * fe[Q + 15:Q + R16] + st
        return 0

    lax.fori_loop(0, E // 512, body, 0)


def _states(xc, dtr, bias, al, e64):
    t = xc.shape[0]
    nc = t // Q
    row = lambda w: pl.BlockSpec((Q, w), lambda i: (i, 0))
    return pl.pallas_call(
        _state_kernel,
        grid=(nc,),
        in_specs=[row(CD), row(H), _const((1, H)), _const((1, H)), _const((Q, E))],
        out_specs=[row(2 * H), pl.BlockSpec((None, 2 * H, Q), lambda i: (i, 0, 0))] + [row(Q)] * 4 + [
                   pl.BlockSpec((None, N, E), lambda i: (i, 0, 0)), pl.BlockSpec((N, E), lambda i: (0, 0)),
                   pl.BlockSpec((R8, H), lambda i: (0, 0))],
        out_shape=[jax.ShapeDtypeStruct((t, 2 * H), F32), jax.ShapeDtypeStruct((nc, 2 * H, Q), F32)]
                  + [jax.ShapeDtypeStruct((t, Q), BF16)] * 4 + [
                   jax.ShapeDtypeStruct((nc, N, E), F32), jax.ShapeDtypeStruct((N, E), F32),
                   jax.ShapeDtypeStruct((R8, H), F32)],
        scratch_shapes=[pltpu.VMEM((Q + R16, Q), BF16)],
        compiler_params=_params(48),
        cost_estimate=_cost(25e9, 70e6),
        name='states',
    )(xc, dtr, bias, al, e64)


def _fwd_kernel(xc_ref, c3_ref, ec3_ref, cdt_ref, hst_ref, hin_ref, z_ref, dyn_ref, d_ref, nw_ref, e_ref, e2_ref,
                yn_ref, dz_ref, dy_ref, hs_ref, dh_ref, gl_ref, row_ref, dnw_ref, dd_ref,
                y_s, sc_a, sc_b, xm_a, xm_b, cb_s, ece, acc1, acc2, p_a, p_b, q_a, q_b):
    i = pl.program_id(0)

    @pl.when(i == 0)
    def _():
        for b in (sc_a, sc_b):
            b[...] = jnp.zeros_like(b)
        ece[...] = jnp.ones_like(ece)
        gl_ref[...] = jnp.zeros_like(gl_ref)
        dnw_ref[...] = jnp.zeros_like(dnw_ref)
        dd_ref[...] = jnp.zeros_like(dd_ref)

    bm = xc_ref[:, E:E + N]
    cm = xc_ref[:, E + N:]
    ct = cm.astype(F32).T.astype(BF16)
    causal = _iota((Q, Q), 0) >= _iota((Q, Q), 1)
    cb_s[...] = jnp.where(causal, _nt(cm, bm), 0.0)
    acc1[...] = jnp.zeros_like(acc1)
    acc2[...] = jnp.zeros_like(acc2)
    head = _iota((1, Q), 1) // H

    def quad(j, sc_s, xm_s):
        L = _lanes(j, Q)
        ej = e_ref[:, L]
        xq = xc_ref[:, L]
        ccol = _dot(c3_ref[...], e2_ref[:, _lanes(j, 512)])
        h = hst_ref[:, L] + ece[0:1, L] * hin_ref[:, L]
        hs_ref[:, L] = h
        yi = _dot(cm, h.astype(BF16)) * _dot(ec3_ref[...], ej)
        for k in range(4):
            crow = cdt_ref[pl.ds(4 * j + k, 1), :]
            drow = cdt_ref[pl.ds(H + 4 * j + k, 1), :]
            cc = ccol[:, k * N:k * N + N]
            for (a, b) in ((0, 0), (1, 0), (1, 1)):
                ra, rb = slice(a * HB, a * HB + HB), slice(b * HB, b * HB + HB)
                seg = jnp.minimum(cc[ra] - crow[:, rb], 0.0)
                w = jnp.exp2(seg) * drow[:, rb]
                sc_s[ra, k * Q + b * HB:k * Q + b * HB + HB] = (cb_s[ra, rb] * w).astype(BF16)
            xm_s[k * Q:k * Q + Q, :] = jnp.where(head == k, xq, jnp.zeros_like(xq))
        y = yi + _dot(sc_s[...], xm_s[...])
        y_s[:, L] = y
        z = z_ref[:, L].astype(F32)
        g = (y + d_ref[:, L] * xq.astype(F32)) * (z * jax.nn.sigmoid(z))
        gg = g * g
        gd = g * (dyn_ref[:, L].astype(F32) * nw_ref[:, L])
        acc1[...] += gg[:, :N] + gg[:, N:]
        acc2[...] += gd[:, :N] + gd[:, N:]

    _twice(quad, (sc_a, xm_a), (sc_b, xm_b))
    r = lax.rsqrt(jnp.sum(acc1[...], 1, keepdims=True) / E + EPS)
    m = jnp.sum(acc2[...], 1, keepdims=True) / E * (r * r * r)
    acc1[...] = jnp.broadcast_to(r, acc1.shape)
    acc2[...] = jnp.broadcast_to(m, acc2.shape)
    row_ref[...] = jnp.zeros_like(row_ref)
    RB = H

    def gate(j, p_s, q_s):
        L = _lanes(j, Q)
        ej = e_ref[:, L]
        ecq = _dot(ec3_ref[...], ej)
        nw = nw_ref[:, L]
        dk = d_ref[:, L]
        dnw = dd = None
        for k in range(Q // RB):
            R = slice(k * RB, k * RB + RB)
            x = xc_ref[R, L].astype(F32)
            ys = y_s[R, L]
            y = ys + dk * x
            z = z_ref[R, L].astype(F32)
            sg = jax.nn.sigmoid(z)
            sz = z * sg
            g = y * sz
            rb = jnp.concatenate([acc1[R, :], acc1[R, :]], 1)
            mb = jnp.concatenate([acc2[R, :], acc2[R, :]], 1)
            gr = g * rb
            dn = dyn_ref[R, L].astype(F32)
            yn_ref[R, L] = (gr * nw).astype(BF16)
            a = jnp.sum((dn * gr).reshape(RB // R8, R8, Q), 0)
            dnw = a if dnw is None else dnw + a
            dg = rb * (dn * nw) - g * mb
            dy = dg * sz
            dz_ref[R, L] = (dg * y * (sg + sz * (1.0 - sg))).astype(BF16)
            dy_ref[R, L] = dy
            a = jnp.sum((dy * x).reshape(RB // R8, R8, Q), 0)
            dd = a if dd is None else dd + a
            hi, lo = _split2(dy.astype(BF16).astype(F32) * ys)
            p_s[R, :] = hi
            p_s[Q + k * RB:Q + k * RB + RB, :] = lo
            q_s[R, :] = (ecq[R] * dy).astype(BF16)
        dnw_ref[:, L] += dnw
        dd_ref[:, L] += dd
        pr = _nt(p_s[...], e_ref[0:2 * H, L])
        row_ref[...] += pr[:Q] + pr[Q:]
        dh = _dot(ct, q_s[...]).astype(BF16)
        dh_ref[:, L] = dh
        gl_ref[:, L] += ece[0:1, L] * dh.astype(F32)
        ece[:, L] = ece[:, L] * ecq[Q - 1:Q]

    _twice(gate, (p_a, q_a), (p_b, q_b))


def _fwd(xc, c3, ec3, cdt, hst, hin, z, dyn, dx, nw, e64, e128):
    t = xc.shape[0]
    nc = t // Q
    row = lambda w: pl.BlockSpec((Q, w), lambda i: (i, 0))
    blk = lambda a, b: pl.BlockSpec((None, a, b), lambda i: (i, 0, 0))
    fix = lambda a, b: pl.BlockSpec((a, b), lambda i: (0, 0))
    return pl.pallas_call(
        _fwd_kernel,
        grid=(nc,),
        in_specs=[row(CD), row(Q), row(Q), blk(2 * H, Q), blk(N, E), _const((N, E)), row(E), row(E), _const((1, E)),
                  _const((1, E)), _const((Q, E)), _const((Q, 2 * E))],
        out_specs=[row(E), row(E), row(E), blk(N, E), blk(N, E), fix(N, E), row(2 * H), fix(R8, E), fix(R8, E)],
        out_shape=[jax.ShapeDtypeStruct((t, E), BF16), jax.ShapeDtypeStruct((t, E), BF16),
                   jax.ShapeDtypeStruct((t, E), F32), jax.ShapeDtypeStruct((nc, N, E), F32),
                   jax.ShapeDtypeStruct((nc, N, E), BF16), jax.ShapeDtypeStruct((N, E), F32),
                   jax.ShapeDtypeStruct((t, 2 * H), F32), jax.ShapeDtypeStruct((R8, E), F32),
                   jax.ShapeDtypeStruct((R8, E), F32)],
        scratch_shapes=[pltpu.VMEM((Q, E), F32)] + [pltpu.VMEM((Q, 4 * Q), BF16)] * 2 + [pltpu.VMEM((4 * Q, Q), BF16)] * 2 + [
                        pltpu.VMEM((Q, Q), F32), pltpu.VMEM((R8, E), F32), pltpu.VMEM((Q, N), F32),
                        pltpu.VMEM((Q, N), F32)] + [pltpu.VMEM((2 * Q, Q), BF16)] * 2 + [pltpu.VMEM((Q, Q), BF16)] * 2,
        compiler_params=_params(60),
        cost_estimate=_cost(150e9, 270e6),
        name='ssd_fwd_gate',
    )(xc, c3, ec3, cdt, hst, hin, z, dyn, dx, nw, e64, e128)


def _bwd_kernel(xc_ref, cd_ref, c3_ref, d3_ref, ec3_ref, f3_ref, cdt_ref, hs_ref, dh_ref, gin_ref, dae_ref, dy_ref, row_ref, d_ref, dtr_ref, bias_ref,
                al_ref, e_ref, e2_ref,
                dxc_ref, ddtr_ref, red_ref,
                g_s, cb_s, dcb_s, dae_s, col_s, db_s, dc_s, sc_a, sc_b, xm_a, xm_b, dm_a, dm_b, w_a, w_b, p_a, p_b):
    i = pl.program_id(0)

    @pl.when(i == 0)
    def _():
        for b in (sc_a, sc_b):
            b[...] = jnp.zeros_like(b)
        g_s[...] = gin_ref[...]
        dae_s[...] = dae_ref[...]
        red_ref[...] = jnp.zeros_like(red_ref)

    dt = cd_ref[:, H:]
    bm = xc_ref[:, E:E + N]
    cm = xc_ref[:, E + N:]
    causal = _iota((Q, Q), 0) <= _iota((Q, Q), 1)
    cb_s[...] = jnp.where(causal, _nt(bm, cm), 0.0)
    dcb_s[...] = jnp.zeros_like(dcb_s)
    col_s[...] = jnp.zeros_like(col_s)
    db_s[...] = jnp.zeros_like(db_s)
    dc_s[...] = jnp.zeros_like(dc_s)
    head = _iota((1, Q), 1) // H
    dae_h = dae_s[0:1, :H]
    dae_s[...] = jnp.zeros_like(dae_s)

    def quad(j, sc_s, xm_s, dm_s, w_s, p_s):
        L = _lanes(j, Q)
        ej = e_ref[:, L]
        xq = xc_ref[:, L]
        dy = dy_ref[:, L]
        dyb = dy.astype(BF16)
        for k in range(4):
            sel = head == k
            xm_s[k * Q:k * Q + Q, :] = jnp.where(sel, xq, jnp.zeros_like(xq))
            dm_s[k * Q:k * Q + Q, :] = jnp.where(sel, dyb, jnp.zeros_like(dyb))
        e2j = e2_ref[:, _lanes(j, 512)]
        ccol = _dot(c3_ref[...], e2j)
        dcol = _dot(d3_ref[...], e2j)
        w_s[...] = _nt(xm_s[...], dyb)
        for k in range(4):
            crow = cdt_ref[pl.ds(4 * j + k, 1), :]
            cc = ccol[:, k * N:k * N + N]
            dc = dcol[:, k * N:k * N + N]
            for (a, b) in ((0, 0), (0, 1), (1, 1)):
                ra, rb = slice(a * HB, a * HB + HB), slice(b * HB, b * HB + HB)
                seg = jnp.minimum(crow[:, rb] - cc[ra], 0.0)
                w = jnp.exp2(seg) * dc[ra]
                sc_s[ra, k * Q + b * HB:k * Q + b * HB + HB] = (cb_s[ra, rb] * w).astype(BF16)
                ds = w_s[k * Q + a * HB:k * Q + a * HB + HB, rb].astype(BF16).astype(F32)
                dcb_s[ra, rb] += ds * w
        dxs = _dot(sc_s[...], dm_s[...])
        fq = _dot(f3_ref[...], ej)
        g = g_s[:, L]
        gb = g.astype(BF16)
        x = xq.astype(F32)
        dxw = _dot(bm, gb).astype(BF16).astype(F32)
        dxs = dxs + fq * dxw
        db_s[...] += _nt((x * fq).astype(BF16), gb)
        ecq = _dot(ec3_ref[...], ej)
        hs = hs_ref[:, L]
        dc_s[...] += _nt((ecq * dy).astype(BF16), hs.astype(BF16))
        hi, lo = _split2(x * dxs)
        p_s[0:Q, :] = hi
        p_s[Q:2 * Q, :] = lo
        dxc_ref[:, L] = (dxs + d_ref[:, L] * dy).astype(BF16)
        gn = g * ecq[Q - 1:Q] + dh_ref[:, L].astype(F32)
        g_s[:, L] = gn
        dr = jnp.broadcast_to(jnp.sum(gn * hs, 0, keepdims=True), (R16, Q))
        hi, lo = _split2(dr)
        p_s[2 * Q:2 * Q + R16, :] = hi
        p_s[2 * Q + R16:2 * Q + 32, :] = lo
        p_s[2 * Q + 32:, :] = (dr - hi.astype(F32) - lo.astype(F32)).astype(BF16)
        pr = _nt(p_s[...], e_ref[0:2 * H, L])
        col_s[...] += pr[:Q] + pr[Q:2 * Q]
        dae_s[...] += pr[2 * Q:2 * Q + R8] + pr[2 * Q + R16:2 * Q + 24] + pr[2 * Q + 32:2 * Q + 40]

    _twice(quad, (sc_a, xm_a, dm_a, w_a, p_a), (sc_b, xm_b, dm_b, w_b, p_b))
    dcb = jnp.where(causal, dcb_s[...], 0.0)
    dxc_ref[:, E:E + N] = (db_s[...] + _dot(dcb.astype(BF16), cm)).astype(BF16)
    dxc_ref[:, E + N:] = (dc_s[...] + _dot(dcb.T.astype(BF16), bm)).astype(BF16)

    col = col_s[:, :H]
    dcs = row_ref[:, :H] - col
    dcs = dcs + jnp.where(_iota((Q, H), 0) == Q - 1, dae_h, 0.0)
    da = _sum3(_dot(causal.astype(BF16), _split3(dcs)))
    na = -jnp.exp(al_ref[...])
    ddt = jnp.where(dt > 0.0, col / jnp.where(dt > 0.0, dt, 1.0), 0.0) + da * na
    ddtr = ddt * jax.nn.sigmoid(dtr_ref[...].astype(F32) + bias_ref[...])
    ddtr_ref[...] = ddtr.astype(BF16)
    both = jnp.concatenate([ddtr, da * (na * dt)], 1)
    red_ref[...] += jnp.sum(both.reshape(Q // R8, R8, 2 * H), 0)


def _bwd(xc, cd, c3, d3, ec3, f3, cdt, hs, dh, gin, dae, dy, row, dx, dtr, bias, al, e64, e128):
    t = xc.shape[0]
    nc = t // Q
    rows = lambda w: pl.BlockSpec((Q, w), lambda i: (nc - 1 - i, 0))
    blk = lambda a, b: pl.BlockSpec((None, a, b), lambda i: (nc - 1 - i, 0, 0))
    fix = lambda a, b: pl.BlockSpec((a, b), lambda i: (0, 0))
    return pl.pallas_call(
        _bwd_kernel,
        grid=(nc,),
        in_specs=[rows(CD), rows(2 * H)] + [rows(Q)] * 4 + [blk(2 * H, Q), blk(N, E), blk(N, E), _const((N, E)), _const((R8, 2 * H)), rows(E),
                  rows(2 * H), _const((1, E)), rows(H), _const((1, H)), _const((1, H)), _const((Q, E)),
                  _const((Q, 2 * E))],
        out_specs=[rows(CD), rows(H), fix(R8, 2 * H)],
        out_shape=[jax.ShapeDtypeStruct((t, CD), BF16), jax.ShapeDtypeStruct((t, H), BF16),
                   jax.ShapeDtypeStruct((R8, 2 * H), F32)],
        scratch_shapes=[pltpu.VMEM((N, E), F32), pltpu.VMEM((Q, Q), F32), pltpu.VMEM((Q, Q), F32), pltpu.VMEM((R8, 2 * H), F32),
                        pltpu.VMEM((Q, 2 * H), F32), pltpu.VMEM((Q, N), F32), pltpu.VMEM((Q, N), F32)]
                       + [pltpu.VMEM((Q, 4 * Q), BF16)] * 2 + [pltpu.VMEM((4 * Q, Q), BF16)] * 4
                       + [pltpu.VMEM((4 * Q, Q), F32)] * 2 + [pltpu.VMEM((2 * Q + 48, Q), BF16)] * 2,
        compiler_params=_params(60),
        cost_estimate=_cost(150e9, 220e6),
        name='ssd_bwd',
    )(xc, cd, c3, d3, ec3, f3, cdt, hs, dh, gin, dae, dy, row, dx, dtr, bias, al, e64, e128)


def _blank(shape):
    return pl.pallas_call(lambda o_ref: None, out_shape=jax.ShapeDtypeStruct(shape, BF16),
                          out_specs=pl.BlockSpec(memory_space=pl.ANY), name='blank')()


def _prefix(s):
    k = s.shape[0]
    cs = jnp.cumsum(s, 0)
    diff = (cs - s)[:, None] - cs[None, :]
    m = (jnp.arange(k)[:, None] > jnp.arange(k)[None, :]).reshape((k, k) + (1,) * (s.ndim - 1))
    return jnp.where(m, jnp.exp(jnp.where(m, diff, 0.0)), 0.0)


def _wide(v):
    return jnp.repeat(v, E // H, axis=-1)


def solution(mesh):
    nseq = mesh.shape['seq']
    fwd = [(i, i + 1) for i in range(nseq - 1)]
    bwd = [(i + 1, i) for i in range(nseq - 1)]
    core = [(i, i ^ 1) for i in range(nseq)]
    chip = [(i, i ^ 2) for i in range(nseq)]

    def layer(x, dout, W_in, conv_w, conv_b, dt_bias, A_log, D_skip, norm_w, W_out):
        t, dm = x.shape
        idx = lax.axis_index('seq')
        c, k = idx % 2, idx // 2
        rows = jnp.arange(Q)
        lane = jnp.arange(2 * E)
        e128 = ((rows[:, None] % H == lane[None, :] // N) & (rows[:, None] < 3 * H)).astype(BF16)
        e64 = ((rows[:, None] % H == lane[None, :E] // H) & (rows[:, None] < 3 * H)).astype(BF16)
        bias, al = dt_bias[None], A_log[None]
        dwide = _wide(D_skip)[None]
        Wz, Wx = W_in[:, :E], W_in[:, E:]

        xb = jnp.dot(x, Wx, preferred_element_type=F32).astype(BF16)
        halo = lax.ppermute(xb[t - R16:], 'seq', fwd)
        dtr = xb[:, CD:]
        xc = _conv_fwd(xb, halo, conv_w, conv_b[None])
        cd, cdt, c3, d3, ec3, f3, hst, h_loc, s8 = _states(xc, dtr, bias, al, e64)
        s = s8[0]
        s_all = lax.all_gather(s, 'seq')
        h_all = lax.all_gather(h_loc, 'seq')
        wd = _wide(_prefix(s_all))
        h_in = jnp.sum(wd[idx][:, None, :] * h_all, 0)
        h_fin = h_loc + _wide(jnp.exp(s))[None] * h_in
        z = jnp.dot(x, Wz, preferred_element_type=F32).astype(BF16)
        dyn = _nt(dout, W_out).astype(BF16)
        yn, dz, dy, hs, dh, g_loc, row, dnw8, dd8 = _fwd(xc, c3, ec3, cdt, hst, h_in, z, dyn, dwide, norm_w[None],
                                                              e64, e128)
        g_all = lax.all_gather(g_loc, 'seq')

        def quarters(a):
            w = a.shape[1] // 4
            cut = lambda cc, kk: lax.dynamic_slice_in_dim(a, (2 * cc + kk) * w, w, 1)
            return (jnp.concatenate([cut(1 - c, 1 - k), cut(1 - c, k)], 1), cut(c, 1 - k), cut(c, k))

        xs, ds = quarters(x), quarters(dout)

        def spread(mine):
            other = lax.ppermute(mine, 'seq', chip)
            mine_p = lax.ppermute(mine, 'seq', core)
            other_p = lax.ppermute(other, 'seq', core)
            return [(2 * c + k, mine), (2 * c + 1 - k, other), (2 - 2 * c + k, mine_p), (3 - 2 * c - k, other_p)]

        w4 = dm // 4
        sO = _tn(yn, ds[0])
        rO = lax.ppermute(sO, 'seq', core)
        sZ = _tn(dz, xs[0])
        rZ = lax.ppermute(sZ, 'seq', core)
        dh_fin = jnp.sum(wd[:, idx][:, None, :] * g_all, 0)
        dae = jnp.sum(jnp.sum(dh_fin * h_fin, 0).reshape(H, E // H), 1)
        dae = jnp.broadcast_to(jnp.concatenate([dae, dae])[None], (R8, 2 * H))
        fO = _tn(yn, ds[1]) + rO[:, :w4]
        gO = lax.ppermute(fO, 'seq', chip)
        fZ = _tn(dz, xs[1]) + rZ[:, :w4]
        gZ = lax.ppermute(fZ, 'seq', chip)
        dxc, ddtr, red = _bwd(xc, cd, c3, d3, ec3, f3, cdt, hs, dh, dh_fin, dae, dy, row, dwide, dtr, bias, al, e64, e128)
        oO = _tn(yn, ds[2]) + rO[:, w4:]
        oZ = _tn(dz, xs[2]) + rZ[:, w4:]
        xe = jnp.concatenate([halo[13:, :CD], xb[:R8, :CD]], 0).astype(F32)
        u = conv_b + sum(conv_w[j] * xe[3 - j:11 - j] for j in range(KCONV))
        sg = jax.nn.sigmoid(u)
        nxt = lax.ppermute(dxc[:R8].astype(F32) * (sg * (1.0 + u * (1.0 - sg))), 'seq', bwd)
        oO, oZ, dxc, gO, nxt = lax.optimization_barrier((oO, oZ, dxc, gO, nxt))
        pO = spread((oO + gO).astype(BF16))
        pZ = spread((oZ + gZ).astype(BF16))
        dxb, gw8, gb8, tail = _conv_bwd(xb, halo, dxc, conv_w, conv_b[None])
        fix = sum(conv_w[j] * jnp.pad(nxt[:j], ((R16 - j, 0), (0, 0))) for j in range(1, KCONV))
        dxb = lax.dynamic_update_slice(dxb, (tail + fix).astype(BF16), (t - R16, 0))
        dxb = lax.dynamic_update_slice(dxb, ddtr, (0, CD))

        dcw = jnp.sum(gw8.reshape(KCONV, R8, CD), 1)
        small = jnp.concatenate([dcw.reshape(-1), jnp.sum(gb8, 0), jnp.sum(red, 0), jnp.sum(dd8, 0).reshape(H, E // H).sum(1),
                                 jnp.sum(dnw8, 0)])
        small = small + lax.ppermute(small, 'seq', core)

        sX = _tn(dxb, xs[0])
        sX, small = lax.optimization_barrier((sX, small))
        rX = lax.ppermute(sX, 'seq', core)
        small = small + lax.ppermute(small, 'seq', chip)
        fX = _tn(dxb, xs[1]) + rX[:, :w4]
        gX = lax.ppermute(fX, 'seq', chip)
        oX = _tn(dxb, xs[2]) + rX[:, w4:]
        dx0 = _nt(dz, Wz)
        dx = (dx0 + _nt(dxb, Wx)).astype(BF16)
        gX, oX, dx = lax.optimization_barrier((gX, oX, dx))
        mX, pO, pZ = lax.optimization_barrier(((oX + gX).astype(BF16), [p for _, p in pO], [p for _, p in pZ]))
        pX = [p for _, p in spread(mX)]
        spots = (2 * c + k, 2 * c + 1 - k, 2 - 2 * c + k, 3 - 2 * c - k)

        def place(out, pieces, row=0):
            for pos, p in zip(spots, pieces):
                out = lax.dynamic_update_slice(out, p, (jnp.int32(row), pos * w4))
            return out

        dW_out = place(_blank((E, dm)), pO)
        dW_in = place(_blank((E + PX, dm)), pZ)
        dW_in = place(dW_in, pX, E).T
        cuts = []
        for n in (KCONV * CD, CD, H, H, H, E):
            cuts.append(small[:n])
            small = small[n:]
        dcw, dcb, ddtb, dal, dD, dnw = cuts
        dcw = dcw.reshape(KCONV, CD)
        return dx, dW_in, dcw, dcb, ddtb, dal, dD, dnw, dW_out

    xs = P(('data', 'seq'), None)
    return jax.shard_map(layer, mesh=mesh, in_specs=(xs, xs) + (P(),) * R8,
                         out_specs=(xs, P('data', None), P('data', None), P('data'), P('data'), P('data'),
                                    P('data'), P('data'), P('data', None)),
                         check_vma=False)
```
